256 devices in a mesh: dp: 128 (over x, z_lo, y, core), tensor: 2 (over z_hi).
Axes of the slice: x: 4, y: 4, z: 8 (z_hi: 2, z_lo: 4; z = z_hi * 4 + z_lo), core: 2. Of those that a mesh axis runs over, the one named last changes fastest.
Arguments:
- activations: bfloat16 [16384, 2048], P('dp', 'tensor'), may hold values from -12 to 12
- dgrad: bfloat16 [16384, 4864], P('dp', 'tensor'), may hold values from -24 to 24
- coding: int32 [128, 4], replicated, may hold values from 0 to 4, as said below
- alive: int32 [128], replicated, may hold values from 0 to 1, as said below
Outputs:
- weight_grad: float32 [2048, 4864], P('dp', 'tensor')
The draws below stay inside these ranges and needn't reach their ends.
Inputs may be any that keep to these rules, and one draw needn't show every extreme that they name: Each entry is 0, 1, 2 or 4; coding[i, 0] is never 0; in each row the zeros come after all nonzero entries; rows 0 to 3 have no zero. Workers 0 to 3 are alive.
All inputs are finite; a program needn't handle non-finite values.
Results may differ from the reference program's by a relative error of at most 0.0003.
Values may be sent and summed in bfloat16 or wider, within the bound.
No kernel may reach another device: no remote copies, remote signals or barrier semaphores. Data moves between devices by JAX's collectives and lax.ppermute only.
A program may use at most 128 MiB of HBM per device.

```python
import math
import jax
import jax.numpy as jnp
from jax import lax

D = 2048
ROWS = 128
SLOTS = 4
FF = 4864
TOKENS = 16384
N_DP = 128


def draw_activations(key, part):
    first, second = jax.random.split(jax.random.fold_in(key, 11), 2)
    row_scale = 10.0 ** jax.random.uniform(second, (TOKENS, 1), jnp.float32, -0.5, 0.5)
    base = jnp.clip(jax.random.normal(first, (TOKENS, D), jnp.float32), -3.5, 3.5)
    return jnp.clip(base * row_scale, -12.0, 12.0).astype(jnp.bfloat16)


def draw_dgrad(key, part):
    first, second, third = jax.random.split(jax.random.fold_in(key, 23), 3)
    row_scale = 10.0 ** jax.random.uniform(second, (TOKENS, 1), jnp.float32, -0.5, 0.5)
    column = jnp.arange(FF, dtype=jnp.float32)[None, :]
    jitter = jnp.exp(jax.random.uniform(third, (1, FF), jnp.float32, -0.5, 0.5))
    column_scale = 4.0 ** (column / FF - 0.5) * jitter
    base = jnp.clip(jax.random.normal(first, (TOKENS, FF), jnp.float32), -3.5, 3.5)
    return jnp.clip(base * row_scale * column_scale, -24.0, 24.0).astype(jnp.bfloat16)


def draw_coding(key, part):
    first, second, third = jax.random.split(jax.random.fold_in(key, 37), 3)
    draws = jax.random.randint(first, (N_DP,), 0, 10)
    counts = 1 + (draws >= 6).astype(jnp.int32) + (draws >= 8).astype(jnp.int32) + (draws >= 9).astype(jnp.int32)
    busiest = jax.random.randint(second, (), 0, N_DP)
    worker = jnp.arange(N_DP)
    counts = jnp.where((worker == busiest) | (worker < SLOTS), SLOTS, jnp.minimum(counts, SLOTS))
    powers = jax.random.randint(third, (N_DP, SLOTS), 0, 3)
    values = jnp.left_shift(jnp.ones((N_DP, SLOTS), jnp.int32), powers)
    slot_index = jnp.arange(SLOTS)[None, :]
    return jnp.where(slot_index < counts[:, None], values, 0).astype(jnp.int32)


def draw_alive(key, part):
    draws = jax.random.randint(jax.random.fold_in(key, 53), (N_DP,), 0, 8)
    worker = jnp.arange(N_DP)
    return jnp.where((draws < 7) | (worker < SLOTS), 1, 0).astype(jnp.int32)


def setup_inputs(seed: int = 0) -> dict:
    arg_keys = jax.random.split(jax.random.key(seed), 5)
    return {
        "activations": draw_activations(jax.random.fold_in(arg_keys[4], 71), 0),
        "dgrad": draw_dgrad(jax.random.fold_in(arg_keys[4], 71), 0),
        "coding": draw_coding(jax.random.fold_in(arg_keys[4], 71), 0),
        "alive": draw_alive(jax.random.fold_in(arg_keys[4], 71), 0),
    }


def pair_products(acts, grads, offset):
    moved_acts = jnp.roll(acts, -offset, axis=0)
    moved_grads = jnp.roll(grads, -offset, axis=0)
    cross_acts = jnp.einsum('pad,pbd->pab', acts, moved_acts, precision=lax.Precision.HIGHEST)
    cross_grads = jnp.einsum('paf,pbf->pab', grads, moved_grads, precision=lax.Precision.HIGHEST)
    return lax.optimization_barrier(jnp.sum(cross_acts * cross_grads, axis=(1, 2)))

def coded_squares(pairs, coefs, slots):
    total = jnp.zeros((coefs.shape[0],), jnp.float32)
    for first in range(slots):
        for second in range(slots):
            lower = min(first, second)
            spread = abs(first - second)
            total = total + coefs[:, first] * coefs[:, second] * jnp.roll(pairs[:, spread], -lower)
    return total

def reference(activations, dgrad, coding, alive):
    workers = N_DP
    acts = activations.astype(jnp.float32).reshape(workers, ROWS, D)
    grads = dgrad.astype(jnp.float32).reshape(workers, ROWS, FF)
    pairs = jnp.stack([pair_products(acts, grads, offset) for offset in range(SLOTS)], axis=1)
    coefs = coding.astype(jnp.float32)
    squares = coded_squares(pairs, coefs, SLOTS)
    limit = 8.0 * math.sqrt(ROWS)
    factor = jnp.minimum(1.0, limit / jnp.sqrt(squares / (D * FF) + 1e-06))
    scaled = alive.astype(jnp.float32) * factor
    weights = jnp.zeros((workers,), jnp.float32)
    for offset in range(SLOTS):
        weights = weights + jnp.roll(scaled * coefs[:, offset], offset)
    weighted = (acts * weights[:, None, None]).reshape(workers * ROWS, D)
    total = jnp.dot(weighted.T, grads.reshape(workers * ROWS, FF), precision=lax.Precision.HIGHEST)
    return total / (limit * math.sqrt(workers))
```

```python
import functools
import math

import jax
import jax.numpy as jnp
from jax import lax
from jax.experimental import pallas as pl
from jax.experimental.pallas import tpu as pltpu
from jax.sharding import Mesh
from jax.sharding import PartitionSpec as P

DP = ("x", "zl", "y", "c")
ALL = (*DP, "t")
BF16 = jnp.bfloat16
F32 = jnp.float32
ROWS = 128
SLOTS = 4
GROUP = 32
EDGE = SLOTS - 1
XW = 256
GW = 640
ANY = pl.BlockSpec(memory_space=pl.ANY)
VMEM = pl.BlockSpec(memory_space=pltpu.VMEM)


def shift(value, axis, by):
    n = lax.axis_size(axis)
    return lax.ppermute(value, axis, [(i, (i + by) % n) for i in range(n)])


def around(value, by):
    place = [(z % 4) * 2 + z // 4 for z in range(8)]
    return lax.ppermute(value, ("zl", "t"), [(place[z], place[(z + by) % 8]) for z in range(8)])


def dot(a, b, dims, **kw):
    return lax.dot_general(a, b, (dims, ((), ())), preferred_element_type=F32, **kw)


def call(kernel, outs, scratch=(), n_in=1, in_specs=None, flops=0, nbytes=0):
    return pl.pallas_call(
        kernel,
        out_shape=[jax.ShapeDtypeStruct(s, d) for s, d in outs],
        in_specs=in_specs or [VMEM] * n_in,
        out_specs=[VMEM] * len(outs),
        scratch_shapes=list(scratch),
        cost_estimate=pl.CostEstimate(flops=flops, bytes_accessed=nbytes, transcendentals=0),
    )


def prologue(x_ref, g_ref, xc_ref, gc_ref):
    x = x_ref[...]
    width = x.shape[1]
    src = lax.broadcasted_iota(jnp.int32, (width, 128), 0)
    col = lax.broadcasted_iota(jnp.int32, (width, 128), 1)
    base = (col // 64) * 512 + ((col % 64) // 16) * 128 + col % 16
    for k in range(8):
        pick = jnp.where(src == base + 16 * k, 1.0, 0.0).astype(BF16)
        xc_ref[k] = dot(x, pick, ((1,), (0,))).astype(BF16)
    width = g_ref.shape[1]
    for n in range(4):
        real = min(GW, width - n * GW)
        gc_ref[n, :, :real] = g_ref[:, n * GW : n * GW + real]
        if real < GW:
            gc_ref[n, :, real:] = jnp.zeros((ROWS, GW - real), BF16)


def assemble(*refs):
    xs, x4, gs = refs[:7], refs[7:9], refs[9:17]
    xt, gt, hout, hkeep, sems = refs[17:]
    zl, y, c = lax.axis_index("zl"), lax.axis_index("y"), lax.axis_index("c")
    z = lax.axis_index("t") * 4 + zl
    copies = []

    def put(src, dst):
        copy = pltpu.make_async_copy(src, dst, sems.at[len(copies)])
        copy.start()
        copies.append(copy)

    def x_place(back):
        at = (z - back + 8) % 8
        return (at % 4) * 1024, (at // 4) * 128

    for back, ref in zip((0, 1, 2, 3, 7, 6, 5), xs):
        row, col = x_place(back)
        put(ref, xt.at[pl.ds(pl.multiple_of(row, 1024), 1024), pl.ds(pl.multiple_of(col, 128), 128)])
    row, col = x_place(4)
    for half in range(2):
        at = pl.multiple_of(row + 512 * half, 512)
        put(x4[half], xt.at[pl.ds(at, 512), pl.ds(pl.multiple_of(col, 128), 128)])

    def g_row(zs, back, core):
        at = zs * 8 + ((y - back + 4) % 4) * 2 + core
        return pl.ds(pl.multiple_of(at * 128, 128), 128)

    for other in range(2):
        core = (c + other) % 2
        own, up, down, far = gs[4 * other : 4 * other + 4]
        for back, ref in ((0, own), (1, up), (3, down), (2, far)):
            for zs in range(4):
                put(ref.at[zs], gt.at[g_row(zs, back, core)])
    for copy in copies:
        copy.wait()
    for ref, at in ((hout, c), (hkeep, 1 - c)):
        rows = pl.ds(pl.multiple_of(at * ((GROUP - EDGE) * ROWS), ROWS), EDGE * ROWS)
        ref[:, :XW] = xt[rows, :]
        ref[:, XW:] = gt[rows, :]


def block_sums(xa, xb, ga, gb):
    gram = dot(xa, xb, ((1,), (1,))) * dot(ga, gb, ((1,), (1,)))
    return jnp.sum(gram.reshape(-1, ROWS, gram.shape[1]), axis=1)


def inner_pairs(xt, gt, v_ref):
    v_ref[...] = jnp.zeros_like(v_ref)

    def step(b, first, count, dynamic):
        rows = pl.ds(pl.multiple_of(first * ROWS, ROWS), count * ROWS) if dynamic else slice(first * ROWS, (first + count) * ROWS)
        cols = pl.ds(pl.multiple_of(b * ROWS, ROWS), 2 * ROWS) if dynamic else slice(b * ROWS, (b + 2) * ROWS)
        sums = block_sums(xt[rows, :], xt[cols, :], gt[rows, :], gt[cols, :])
        for s in range(2):
            for r in range(count):
                d = count - 2 + s - r
                if 0 <= d < SLOTS:
                    v_ref[pl.ds(d * GROUP + first + r, 1), :] = sums[r : r + 1, s * ROWS : (s + 1) * ROWS]

    step(0, 0, 2, False)
    step(2, 0, 4, False)

    def body(j, carry):
        step(2 * j, 2 * j - 3, 5, True)
        return carry

    lax.fori_loop(2, GROUP // 2, body, 0, unroll=2)


def edge_pairs(v_ref, keep, got, out_ref, v):
    v[...] = v_ref[...]
    first = lax.axis_index("c") == 0
    sums = block_sums(keep[:, :XW], got[:, :XW], keep[:, XW:], got[:, XW:])

    def pair(i, j):
        return sums[i : i + 1, j * ROWS : (j + 1) * ROWS]

    for e in range(EDGE):
        for f in range(e + 1):
            at = (EDGE + f - e) * GROUP + GROUP - EDGE + e
            v[at : at + 1, :] = jnp.where(first, pair(e, f), pair(f, e))
    total = dot(jnp.ones((8, ROWS), F32), v[...], ((1,), (1,)), precision=lax.Precision.HIGHEST)
    out_ref[...] = jnp.broadcast_to(total[0:1].reshape(1, 1, ROWS), out_ref.shape)


def weigh(size, r_ref, coding_ref, alive_ref, xt, gt, *refs):
    outs, (acc, hi, lo) = refs[:4], refs[4:]
    x = lax.axis_index("x")
    workers = ROWS
    limit = 8.0 * math.sqrt(ROWS)
    parts = r_ref[...].reshape(4, 16, 2, 2, 1, 128)
    even = jnp.sum(parts[:, :, 0], axis=(1, 2))
    odd = jnp.sum(parts[:, :, 1], axis=(1, 2))
    lane = lax.broadcasted_iota(jnp.int32, (8, 128), 1)
    edge = (lane % GROUP) + lane // GROUP >= GROUP

    def full(row):
        return jnp.broadcast_to(row, (8, 128))

    groups = [full(even[i]) + jnp.where(edge, full(odd[(i + 1) % 4]), full(odd[i])) for i in range(4)]

    def turn(value, by):
        by = by % 128
        return value if by == 0 else pltpu.roll(value, by, 1)

    pairs = []
    for d in range(SLOTS):
        value = jnp.zeros((8, 128), F32)
        for i in range(4):
            value = jnp.where(lane // GROUP == i, turn(groups[i], GROUP * (i - d)), value)
        pairs.append(value)
    coef = [full(coding_ref[s : s + 1, :].astype(F32)) for s in range(SLOTS)]
    squares = jnp.zeros((8, 128), F32)
    for s in range(SLOTS):
        for u in range(s, SLOTS):
            squares += (1.0 if u == s else 2.0) * coef[s] * coef[u] * turn(pairs[u - s], -s)
    squares = jnp.maximum(squares, 0.0)
    factor = jnp.minimum(1.0, limit / jnp.sqrt(squares / size + 1e-6))
    scaled = full(alive_ref[...].astype(F32)) * factor * (1.0 / (limit * math.sqrt(workers)))
    weights = jnp.zeros((8, 128), F32)
    for s in range(SLOTS):
        weights += turn(scaled * coef[s], s)
    mine = pltpu.roll(weights, ((4 - x) % 4) * GROUP, 1)[0:1]
    for chunk in range(4):
        for q in range(8):
            at = chunk * 8 + q
            value = xt[at * ROWS : (at + 1) * ROWS, :].astype(F32) * mine[:, at : at + 1]
            top = value.astype(BF16)
            hi[q * ROWS : (q + 1) * ROWS, :] = top
            lo[q * ROWS : (q + 1) * ROWS, :] = (value - top.astype(F32)).astype(BF16)
        g = gt[chunk * 1024 : (chunk + 1) * 1024, :]
        new = dot(hi[...], g, ((0,), (0,))) + dot(lo[...], g, ((0,), (0,)))
        acc[...] = new if chunk == 0 else acc[...] + new
    for k in range(4):
        outs[k][...] = acc[pl.ds(pl.multiple_of(((x + k) % 4) * 64, 64), 64), :]


def local(activations, dgrad, coding, alive):
    size = float(activations.shape[1] * 2) * float(dgrad.shape[1] * 2)
    xc, gc = call(
        prologue, [((8, ROWS, 128), BF16), ((4, ROWS, GW), BF16)], n_in=2, flops=1 << 28, nbytes=1 << 21
    )(activations, dgrad)
    gz = lax.all_to_all(gc, "zl", 0, 0, tiled=True)
    xa = lax.all_to_all(xc, ("y", "c"), 0, 0, tiled=True).reshape(8 * ROWS, 128)
    up = shift(gz, "y", 1)
    down = shift(gz, "y", -1)
    xs_up, xs_down = [], []
    a, b = xa, xa
    for _ in range(3):
        a, b = around(a, 1), around(b, -1)
        xs_up.append(a)
        xs_down.append(b)
    far_top = shift(up[:2], "y", 1)
    far_bottom = shift(down[2:], "y", -1)
    x4 = [around(a[: 4 * ROWS], 1), around(b[4 * ROWS :], -1)]
    far = jnp.concatenate([far_top, far_bottom], axis=0)
    mine = [gz, up, down, far]
    theirs = [shift(v, "c", 1) for v in mine]
    tokens = GROUP * ROWS
    xt, gt, hout, hkeep = call(
        assemble,
        [((tokens, XW), BF16), ((tokens, GW), BF16), ((EDGE * ROWS, XW + GW), BF16), ((EDGE * ROWS, XW + GW), BF16)],
        scratch=[pltpu.SemaphoreType.DMA((41,))],
        in_specs=[ANY] * 17,
        nbytes=1 << 24,
    )(xa, *xs_up, *xs_down, *x4, *mine, *theirs)
    way = []
    for i in range(4):
        way += [(i * 2, (i + 3) % 4 * 2), (i * 2 + 1, (i + 1) % 4 * 2 + 1)]
    got = lax.ppermute(hout, ("x", "c"), way)
    (v,) = call(inner_pairs, [((128, 128), F32)], n_in=2, flops=1 << 32, nbytes=1 << 23)(xt, gt)
    (sums,) = call(
        edge_pairs, [((256, 1, 128), F32)], scratch=[pltpu.VMEM((128, 128), F32)], n_in=3, flops=1 << 28, nbytes=1 << 20
    )(v, hkeep, got)
    sums = lax.all_to_all(sums, ALL, 0, 0, tiled=True)
    parts = call(
        functools.partial(weigh, size),
        [((64, GW), F32)] * 4,
        scratch=[pltpu.VMEM((XW, GW), F32), pltpu.VMEM((1024, XW), BF16), pltpu.VMEM((1024, XW), BF16)],
        n_in=5,
        flops=1 << 31,
        nbytes=1 << 23,
    )(sums, coding.T, alive.reshape(1, -1), xt, gt)
    total = parts[0]
    for k in range(1, 4):
        total = total + shift(parts[k], "x", k)
    tiles = lax.all_to_all(total.reshape(4, 16, GW), "zl", 0, 0, tiled=True)
    return jnp.concatenate([tiles[i] for i in range(4)], axis=1)[:, : dgrad.shape[1]]


def solution(mesh):
    finer = Mesh(mesh.devices.reshape(4, 4, 4, 2, 2), ALL)
    placed = (P(DP, "t"), P(DP, "t"), P(), P())
    return jax.shard_map(local, mesh=finer, in_specs=placed, out_specs=P(DP, "t"), check_vma=False)
```

```python
import functools
import math

import jax
import jax.numpy as jnp
from jax import lax
from jax.experimental import pallas as pl
from jax.experimental.pallas import tpu as pltpu
from jax.sharding import Mesh
from jax.sharding import PartitionSpec as P

DP = ("x", "zl", "y", "c")
ALL = (*DP, "t")
BF16 = jnp.bfloat16
F32 = jnp.float32
ROWS = 128
SLOTS = 4
GROUP = 32
EDGE = SLOTS - 1
XW = 256
GW = 640
ANY = pl.BlockSpec(memory_space=pl.ANY)
VMEM = pl.BlockSpec(memory_space=pltpu.VMEM)


def shift(value, axis, by):
    n = lax.axis_size(axis)
    return lax.ppermute(value, axis, [(i, (i + by) % n) for i in range(n)])


def around(value, by):
    place = [(z % 4) * 2 + z // 4 for z in range(8)]
    return lax.ppermute(value, ("zl", "t"), [(place[z], place[(z + by) % 8]) for z in range(8)])


def dot(a, b, dims, **kw):
    return lax.dot_general(a, b, (dims, ((), ())), preferred_element_type=F32, **kw)


def call(kernel, outs, scratch=(), n_in=1, in_specs=None, flops=0, nbytes=0, mib=16):
    return pl.pallas_call(
        kernel,
        out_shape=[jax.ShapeDtypeStruct(s, d) for s, d in outs],
        in_specs=in_specs or [VMEM] * n_in,
        out_specs=[VMEM] * len(outs),
        scratch_shapes=list(scratch),
        cost_estimate=pl.CostEstimate(flops=flops, bytes_accessed=nbytes, transcendentals=0),
        compiler_params=pltpu.CompilerParams(vmem_limit_bytes=mib << 20),
    )


def prologue(x_ref, g_ref, xc_ref, *refs):
    gc, wide = refs[:4], refs[4]
    x = x_ref[...]
    width = x.shape[1]
    src = lax.broadcasted_iota(jnp.int32, (width, 128), 0)
    col = lax.broadcasted_iota(jnp.int32, (width, 128), 1)
    base = (col // 64) * 512 + ((col % 64) // 16) * 128 + col % 16
    for k in range(8):
        pick = jnp.where(src == base + 16 * k, 1.0, 0.0).astype(BF16)
        xc_ref[k] = dot(x, pick, ((1,), (0,))).astype(BF16)
    width = g_ref.shape[1]
    wide[:, :width] = g_ref[...]
    wide[:, width:] = jnp.zeros((ROWS, 4 * GW - width), BF16)
    zl = lax.axis_index("zl")
    for k in range(4):
        gc[k][...] = wide[:, pl.ds(pl.multiple_of(((zl + k) % 4) * GW, 128), GW)]


def assemble(*refs):
    xs, x4, gs = refs[:7], refs[7:9], refs[9:25]
    xt, gt, hout, hkeep, sems = refs[25:]
    zl, y, c = lax.axis_index("zl"), lax.axis_index("y"), lax.axis_index("c")
    z = lax.axis_index("t") * 4 + zl
    copies = []

    def put(src, dst):
        copy = pltpu.make_async_copy(src, dst, sems.at[len(copies)])
        copy.start()
        copies.append(copy)

    def x_place(back):
        at = (z - back + 8) % 8
        return (at % 4) * 1024, (at // 4) * 128

    for back, ref in zip((0, 1, 2, 3, 7, 6, 5), xs):
        row, col = x_place(back)
        put(ref, xt.at[pl.ds(pl.multiple_of(row, 1024), 1024), pl.ds(pl.multiple_of(col, 128), 128)])
    row, col = x_place(4)
    for half in range(2):
        at = pl.multiple_of(row + 512 * half, 512)
        put(x4[half], xt.at[pl.ds(at, 512), pl.ds(pl.multiple_of(col, 128), 128)])

    def g_row(zs, back, core):
        at = zs * 8 + ((y - back + 4) % 4) * 2 + core
        return pl.ds(pl.multiple_of(at * 128, 128), 128)

    for other in range(2):
        core = (c + other) % 2
        for i, back in enumerate((0, 1, 3, 2)):
            for k in range(4):
                piece = gs[8 * other + 2 * i + k // 2]
                put(piece.at[k % 2], gt.at[g_row((zl - k + 4) % 4, back, core)])
    for copy in copies:
        copy.wait()
    for ref, at in ((hout, c), (hkeep, 1 - c)):
        rows = pl.ds(pl.multiple_of(at * ((GROUP - EDGE) * ROWS), ROWS), EDGE * ROWS)
        ref[:, :XW] = xt[rows, :]
        ref[:, XW:] = gt[rows, :]


def block_sums(xa, xb, ga, gb):
    gram = dot(xa, xb, ((1,), (1,))) * dot(ga, gb, ((1,), (1,)))
    return jnp.sum(gram.reshape(-1, ROWS, gram.shape[1]), axis=1)


def inner_pairs(xt, gt, v_ref):
    v_ref[...] = jnp.zeros_like(v_ref)

    def step(b, first, count, dynamic):
        rows = pl.ds(pl.multiple_of(first * ROWS, ROWS), count * ROWS) if dynamic else slice(first * ROWS, (first + count) * ROWS)
        cols = pl.ds(pl.multiple_of(b * ROWS, ROWS), 2 * ROWS) if dynamic else slice(b * ROWS, (b + 2) * ROWS)
        sums = block_sums(xt[rows, :], xt[cols, :], gt[rows, :], gt[cols, :])
        for s in range(2):
            for r in range(count):
                d = count - 2 + s - r
                if 0 <= d < SLOTS:
                    v_ref[pl.ds(d * GROUP + first + r, 1), :] = sums[r : r + 1, s * ROWS : (s + 1) * ROWS]

    step(0, 0, 2, False)
    step(2, 0, 4, False)

    def body(j, carry):
        step(2 * j, 2 * j - 3, 5, True)
        return carry

    lax.fori_loop(2, GROUP // 2, body, 0, unroll=2)


def edge_pairs(v_ref, keep, got, out_ref, v):
    v[...] = v_ref[...]
    first = lax.axis_index("c") == 0
    sums = block_sums(keep[:, :XW], got[:, :XW], keep[:, XW:], got[:, XW:])

    def pair(i, j):
        return sums[i : i + 1, j * ROWS : (j + 1) * ROWS]

    for e in range(EDGE):
        for f in range(e + 1):
            at = (EDGE + f - e) * GROUP + GROUP - EDGE + e
            v[at : at + 1, :] = jnp.where(first, pair(e, f), pair(f, e))
    total = dot(jnp.ones((8, ROWS), F32), v[...], ((1,), (1,)), precision=lax.Precision.HIGHEST)
    out_ref[...] = jnp.broadcast_to(total[0:1].reshape(1, 1, ROWS), out_ref.shape)


def weigh(size, r_ref, coding_ref, alive_ref, xt, gt, *refs):
    outs, (acc, hi, lo) = refs[:4], refs[4:]
    x = lax.axis_index("x")
    workers = ROWS
    limit = 8.0 * math.sqrt(ROWS)
    parts = r_ref[...].reshape(4, 16, 2, 2, 1, 128)
    even = jnp.sum(parts[:, :, 0], axis=(1, 2))
    odd = jnp.sum(parts[:, :, 1], axis=(1, 2))
    lane = lax.broadcasted_iota(jnp.int32, (8, 128), 1)
    edge = (lane % GROUP) + lane // GROUP >= GROUP

    def full(row):
        return jnp.broadcast_to(row, (8, 128))

    groups = [full(even[i]) + jnp.where(edge, full(odd[(i + 1) % 4]), full(odd[i])) for i in range(4)]

    def turn(value, by):
        by = by % 128
        return value if by == 0 else pltpu.roll(value, by, 1)

    pairs = []
    for d in range(SLOTS):
        value = jnp.zeros((8, 128), F32)
        for i in range(4):
            value = jnp.where(lane // GROUP == i, turn(groups[i], GROUP * (i - d)), value)
        pairs.append(value)
    coef = [full(coding_ref[s : s + 1, :].astype(F32)) for s in range(SLOTS)]
    squares = jnp.zeros((8, 128), F32)
    for s in range(SLOTS):
        for u in range(s, SLOTS):
            squares += (1.0 if u == s else 2.0) * coef[s] * coef[u] * turn(pairs[u - s], -s)
    squares = jnp.maximum(squares, 0.0)
    factor = jnp.minimum(1.0, limit / jnp.sqrt(squares / size + 1e-6))
    scaled = full(alive_ref[...].astype(F32)) * factor * (1.0 / (limit * math.sqrt(workers)))
    weights = jnp.zeros((8, 128), F32)
    for s in range(SLOTS):
        weights += turn(scaled * coef[s], s)
    mine = pltpu.roll(weights, ((4 - x) % 4) * GROUP, 1)[0:1]
    for chunk in range(4):
        for q in range(8):
            at = chunk * 8 + q
            value = xt[at * ROWS : (at + 1) * ROWS, :].astype(F32) * mine[:, at : at + 1]
            top = value.astype(BF16)
            hi[q * ROWS : (q + 1) * ROWS, :] = top
            lo[q * ROWS : (q + 1) * ROWS, :] = (value - top.astype(F32)).astype(BF16)
        g = gt[chunk * 1024 : (chunk + 1) * 1024, :]
        new = dot(hi[...], g, ((0,), (0,))) + dot(lo[...], g, ((0,), (0,)))
        acc[...] = new if chunk == 0 else acc[...] + new
    for k in range(4):
        outs[k][...] = acc[pl.ds(pl.multiple_of(((x + k) % 4) * 64, 64), 64), :]


def local(activations, dgrad, coding, alive):
    size = float(activations.shape[1] * 2) * float(dgrad.shape[1] * 2)
    xc, *gc = call(
        prologue,
        [((8, ROWS, 128), BF16)] + [((ROWS, GW), BF16)] * 4,
        scratch=[pltpu.VMEM((ROWS, 4 * GW), BF16)],
        n_in=2,
        flops=1 << 28,
        nbytes=1 << 21,
    )(activations, dgrad)
    gs = [gc[0]] + [shift(gc[k], "zl", k) for k in (1, 2, 3)]
    gz = [jnp.stack(gs[:2]), jnp.stack(gs[2:])]
    xa = lax.all_to_all(xc, ("y", "c"), 0, 0, tiled=True).reshape(8 * ROWS, 128)
    up = [shift(v, "y", 1) for v in gz]
    down = [shift(v, "y", -1) for v in gz]
    xs_up, xs_down = [], []
    a, b = xa, xa
    for _ in range(3):
        a, b = around(a, 1), around(b, -1)
        xs_up.append(a)
        xs_down.append(b)
    far = [shift(up[0], "y", 1), shift(down[1], "y", -1)]
    x4 = [around(a[: 4 * ROWS], 1), around(b[4 * ROWS :], -1)]
    mine = gz + up + down + far
    theirs = [shift(v, "c", 1) for v in mine]
    tokens = GROUP * ROWS
    xt, gt, hout, hkeep = call(
        assemble,
        [((tokens, XW), BF16), ((tokens, GW), BF16), ((EDGE * ROWS, XW + GW), BF16), ((EDGE * ROWS, XW + GW), BF16)],
        scratch=[pltpu.SemaphoreType.DMA((41,))],
        in_specs=[ANY] * 25,
        nbytes=1 << 24,
    )(xa, *xs_up, *xs_down, *x4, *mine, *theirs)
    way = []
    for i in range(4):
        way += [(i * 2, (i + 3) % 4 * 2), (i * 2 + 1, (i + 1) % 4 * 2 + 1)]
    got = lax.ppermute(hout, ("x", "c"), way)
    (v,) = call(inner_pairs, [((128, 128), F32)], n_in=2, flops=1 << 32, nbytes=1 << 23)(xt, gt)
    (sums,) = call(
        edge_pairs, [((256, 1, 128), F32)], scratch=[pltpu.VMEM((128, 128), F32)], n_in=3, flops=1 << 28, nbytes=1 << 20
    )(v, hkeep, got)
    sums = lax.all_to_all(sums, ALL, 0, 0, tiled=True)
    parts = call(
        functools.partial(weigh, size),
        [((64, GW), F32)] * 4,
        scratch=[pltpu.VMEM((XW, GW), F32), pltpu.VMEM((1024, XW), BF16), pltpu.VMEM((1024, XW), BF16)],
        n_in=5,
        flops=1 << 31,
        nbytes=1 << 23,
    )(sums, coding.T, alive.reshape(1, -1), xt, gt)
    total = parts[0]
    for k in range(1, 4):
        total = total + shift(parts[k], "x", k)
    tiles = lax.all_to_all(total.reshape(4, 16, GW), "zl", 0, 0, tiled=True)
    return jnp.concatenate([tiles[i] for i in range(4)], axis=1)[:, : dgrad.shape[1]]


def solution(mesh):
    finer = Mesh(mesh.devices.reshape(4, 4, 4, 2, 2), ALL)
    placed = (P(DP, "t"), P(DP, "t"), P(), P())
    return jax.shard_map(local, mesh=finer, in_specs=placed, out_specs=P(DP, "t"), check_vma=False)
```

```python
import functools
import math

import jax
import jax.numpy as jnp
from jax import lax
from jax.experimental import pallas as pl
from jax.experimental.pallas import tpu as pltpu
from jax.sharding import Mesh
from jax.sharding import PartitionSpec as P

DP = ("x", "zl", "y", "c")
ALL = (*DP, "t")
BF16 = jnp.bfloat16
F32 = jnp.float32
ROWS = 128
SLOTS = 4
GROUP = 32
EDGE = SLOTS - 1
XW = 256
GW = 640
VMEM = pl.BlockSpec(memory_space=pltpu.VMEM)


def shift(value, axis, by):
    n = lax.axis_size(axis)
    return lax.ppermute(value, axis, [(i, (i + by) % n) for i in range(n)])


def around(value, by):
    place = [(z % 4) * 2 + z // 4 for z in range(8)]
    return lax.ppermute(value, ("zl", "t"), [(place[z], place[(z + by) % 8]) for z in range(8)])


def dot(a, b, dims, **kw):
    return lax.dot_general(a, b, (dims, ((), ())), preferred_element_type=F32, **kw)


def call(kernel, outs, scratch=(), n_in=1, in_specs=None, flops=0, nbytes=0, mib=16):
    return pl.pallas_call(
        kernel,
        out_shape=[jax.ShapeDtypeStruct(s, d) for s, d in outs],
        in_specs=in_specs or [VMEM] * n_in,
        out_specs=[VMEM] * len(outs),
        scratch_shapes=list(scratch),
        cost_estimate=pl.CostEstimate(flops=flops, bytes_accessed=nbytes, transcendentals=0),
        compiler_params=pltpu.CompilerParams(vmem_limit_bytes=mib << 20),
    )


def split_x(x_ref, xc_ref):
    x = x_ref[...]
    width = x.shape[1]
    src = lax.broadcasted_iota(jnp.int32, (width, 128), 0)
    col = lax.broadcasted_iota(jnp.int32, (width, 128), 1)
    base = (col // 64) * 512 + ((col % 64) // 16) * 128 + col % 16
    for k in range(8):
        pick = jnp.where(src == base + 16 * k, 1.0, 0.0).astype(BF16)
        xc_ref[k] = dot(x, pick, ((1,), (0,))).astype(BF16)


def split_g(g_ref, *refs):
    gc, wide = refs[:4], refs[4]
    width = g_ref.shape[1]
    wide[:, :width] = g_ref[...]
    wide[:, width:] = jnp.zeros((ROWS, 4 * GW - width), BF16)
    zl = lax.axis_index("zl")
    for k in range(4):
        gc[k][...] = wide[:, pl.ds(pl.multiple_of(((zl + k) % 4) * GW, 128), GW)]


def assemble(places, *refs):
    xs, gs = refs[: len(places[0])], refs[len(places[0]) : -4]
    xt, gt, hout, hkeep = refs[-4:]
    zl, y, c = lax.axis_index("zl"), lax.axis_index("y"), lax.axis_index("c")
    z = lax.axis_index("t") * 4 + zl
    for (back, half), ref in zip(places[0], xs):
        at = (z - back + 8) % 8
        rows = pl.ds(pl.multiple_of((at % 4) * 1024 + half, 512), ref.shape[0])
        xt[rows, pl.ds(pl.multiple_of((at // 4) * 128, 128), 128)] = ref[...]
    for (back, first, other), ref in zip(places[1], gs):
        core = (c + other) % 2
        for k in range(ref.shape[0] // ROWS):
            at = ((zl - first - k + 4) % 4) * 8 + ((y - back + 4) % 4) * 2 + core
            gt[pl.ds(pl.multiple_of(at * ROWS, ROWS), ROWS), :] = ref[k * ROWS : (k + 1) * ROWS, :]
    for ref, at in ((hout, c), (hkeep, 1 - c)):
        rows = pl.ds(pl.multiple_of(at * ((GROUP - EDGE) * ROWS), ROWS), EDGE * ROWS)
        ref[:, :XW] = xt[rows, :]
        ref[:, XW:] = gt[rows, :]


def block_sums(xa, xb, ga, gb):
    gram = dot(xa, xb, ((1,), (1,))) * dot(ga, gb, ((1,), (1,)))
    return jnp.sum(gram.reshape(-1, ROWS, gram.shape[1]), axis=1)


def inner_pairs(xt, gt, v_ref):
    v_ref[...] = jnp.zeros_like(v_ref)

    def step(b, first, count, dynamic):
        rows = pl.ds(pl.multiple_of(first * ROWS, ROWS), count * ROWS) if dynamic else slice(first * ROWS, (first + count) * ROWS)
        cols = pl.ds(pl.multiple_of(b * ROWS, ROWS), 2 * ROWS) if dynamic else slice(b * ROWS, (b + 2) * ROWS)
        sums = block_sums(xt[rows, :], xt[cols, :], gt[rows, :], gt[cols, :])
        for s in range(2):
            for r in range(count):
                d = count - 2 + s - r
                if 0 <= d < SLOTS:
                    v_ref[pl.ds(d * GROUP + first + r, 1), :] = sums[r : r + 1, s * ROWS : (s + 1) * ROWS]

    step(0, 0, 2, False)
    step(2, 0, 4, False)

    def body(j, carry):
        step(2 * j, 2 * j - 3, 5, True)
        return carry

    lax.fori_loop(2, GROUP // 2, body, 0, unroll=2)


def edge_pairs(v_ref, keep, got, out_ref, v):
    v[...] = v_ref[...]
    first = lax.axis_index("c") == 0
    sums = block_sums(keep[:, :XW], got[:, :XW], keep[:, XW:], got[:, XW:])

    def pair(i, j):
        return sums[i : i + 1, j * ROWS : (j + 1) * ROWS]

    for e in range(EDGE):
        for f in range(e + 1):
            at = (EDGE + f - e) * GROUP + GROUP - EDGE + e
            v[at : at + 1, :] = jnp.where(first, pair(e, f), pair(f, e))
    total = dot(jnp.ones((8, ROWS), F32), v[...], ((1,), (1,)), precision=lax.Precision.HIGHEST)
    out_ref[...] = jnp.broadcast_to(total[0:1].reshape(1, 1, ROWS), out_ref.shape)


def weigh(size, r_ref, coding_ref, alive_ref, xt, gt, *refs):
    outs, (acc, hi, lo) = refs[:4], refs[4:]
    x = lax.axis_index("x")
    workers = ROWS
    limit = 8.0 * math.sqrt(ROWS)
    parts = r_ref[...].reshape(4, 16, 2, 2, 1, 128)
    even = jnp.sum(parts[:, :, 0], axis=(1, 2))
    odd = jnp.sum(parts[:, :, 1], axis=(1, 2))
    lane = lax.broadcasted_iota(jnp.int32, (8, 128), 1)
    edge = (lane % GROUP) + lane // GROUP >= GROUP

    def full(row):
        return jnp.broadcast_to(row, (8, 128))

    groups = [full(even[i]) + jnp.where(edge, full(odd[(i + 1) % 4]), full(odd[i])) for i in range(4)]

    def turn(value, by):
        by = by % 128
        return value if by == 0 else pltpu.roll(value, by, 1)

    pairs = []
    for d in range(SLOTS):
        value = jnp.zeros((8, 128), F32)
        for i in range(4):
            value = jnp.where(lane // GROUP == i, turn(groups[i], GROUP * (i - d)), value)
        pairs.append(value)
    coef = [full(coding_ref[s : s + 1, :].astype(F32)) for s in range(SLOTS)]
    squares = jnp.zeros((8, 128), F32)
    for s in range(SLOTS):
        for u in range(s, SLOTS):
            squares += (1.0 if u == s else 2.0) * coef[s] * coef[u] * turn(pairs[u - s], -s)
    squares = jnp.maximum(squares, 0.0)
    factor = jnp.minimum(1.0, limit / jnp.sqrt(squares / size + 1e-6))
    scaled = full(alive_ref[...].astype(F32)) * factor * (1.0 / (limit * math.sqrt(workers)))
    weights = jnp.zeros((8, 128), F32)
    for s in range(SLOTS):
        weights += turn(scaled * coef[s], s)
    mine = pltpu.roll(weights, ((4 - x) % 4) * GROUP, 1)
    acc[...] = jnp.zeros_like(acc)

    def chunk(i, mine):
        for q in range(8):
            rows = pl.ds(pl.multiple_of((i * 8 + q) * ROWS, ROWS), ROWS)
            value = xt[rows, :].astype(F32) * mine[0:1, q : q + 1]
            top = value.astype(BF16)
            hi[q * ROWS : (q + 1) * ROWS, :] = top
            lo[q * ROWS : (q + 1) * ROWS, :] = (value - top.astype(F32)).astype(BF16)
        g = gt[pl.ds(pl.multiple_of(i * 1024, 1024), 1024), :]
        acc[...] += dot(hi[...], g, ((0,), (0,))) + dot(lo[...], g, ((0,), (0,)))
        return pltpu.roll(mine, 120, 1)

    lax.fori_loop(0, 4, chunk, mine, unroll=2)
    for k in range(4):
        outs[k][...] = acc[pl.ds(pl.multiple_of(((x + k) % 4) * 64, 64), 64), :]


def add_up(a, b, c, d, *outs):
    zl = lax.axis_index("zl")
    for k in range(4):
        rows = pl.ds(pl.multiple_of(((zl + k) % 4) * 16, 16), 16)
        outs[k][...] = a[rows, :] + b[rows, :] + c[rows, :] + d[rows, :]


def lay_out(*refs):
    parts, out_ref, wide = refs[:4], refs[4], refs[5]
    zl = lax.axis_index("zl")
    for k in range(4):
        wide[:, pl.ds(pl.multiple_of(((zl - k + 4) % 4) * GW, 128), GW)] = parts[k][...]
    out_ref[...] = wide[:, : out_ref.shape[1]]


def steps(activations, dgrad, coding, alive):
    size = float(activations.shape[1] * 2) * float(dgrad.shape[1] * 2)
    columns = dgrad.shape[1]
    (xc,) = call(split_x, [((8, ROWS, 128), BF16)], flops=1 << 28, nbytes=1 << 20)(activations)
    xa = functools.partial(lax.all_to_all, tiled=True)(xc, ("y", "c"), 0, 0).reshape(8 * ROWS, 128)
    gc = call(
        split_g, [((ROWS, GW), BF16)] * 4, scratch=[pltpu.VMEM((ROWS, 4 * GW), BF16)], flops=1 << 16, nbytes=1 << 21
    )(dgrad)
    g = [gc[0]] + [shift(gc[k], "zl", k) for k in (1, 2, 3)]
    near, late = jnp.concatenate(g[:2], axis=0), jnp.concatenate(g[2:], axis=0)
    pieces = {}
    for name, first, own in (("A", 0, near), ("B", 2, late)):
        pieces[f"own{name}"] = (own, 0, first)
        pieces[f"up{name}"] = (shift(own, "y", 1), 1, first)
        pieces[f"down{name}"] = (shift(own, "y", -1), 3, first)
    pieces["farA"] = (shift(pieces["upA"][0], "y", 1), 2, 0)
    pieces["farB"] = (shift(pieces["downB"][0], "y", -1), 2, 2)
    gs = [v for v, _, _ in pieces.values()]
    g_places = [(back, first, 0) for _, back, first in pieces.values()]
    gs += [shift(v, "c", 1) for (v, _, _) in pieces.values()]
    g_places += [(back, first, 1) for _, back, first in pieces.values()]
    xs, x_places = [xa], [(0, 0)]
    for sign, way in ((1, "up"), (-1, "down")):
        value = xa
        for step in range(1, 5):
            half = 0
            if step == 4:
                half = 0 if sign == 1 else 512
                value = value[half : half + 512]
            value = around(value, sign)
            xs.append(value)
            x_places.append(((sign * step) % 8, half))
    tokens = GROUP * ROWS
    xt, gt, hout, hkeep = call(
        functools.partial(assemble, (x_places, g_places)),
        [((tokens, XW), BF16), ((tokens, GW), BF16), ((EDGE * ROWS, XW + GW), BF16), ((EDGE * ROWS, XW + GW), BF16)],
        n_in=len(xs) + len(gs),
        nbytes=1 << 24,
    )(*xs, *gs)
    way = []
    for i in range(4):
        way += [(i * 2, (i + 3) % 4 * 2), (i * 2 + 1, (i + 1) % 4 * 2 + 1)]
    got = lax.ppermute(hout, ("x", "c"), way)
    (v,) = call(inner_pairs, [((128, 128), F32)], n_in=2, flops=1 << 32, nbytes=1 << 23)(xt, gt)
    (sums,) = call(
        edge_pairs, [((256, 1, 128), F32)], scratch=[pltpu.VMEM((128, 128), F32)], n_in=3, flops=1 << 28, nbytes=1 << 20
    )(v, hkeep, got)
    sums = lax.all_to_all(sums, ALL, 0, 0, tiled=True)
    parts = call(
        functools.partial(weigh, size),
        [((64, GW), F32)] * 4,
        scratch=[pltpu.VMEM((XW, GW), F32), pltpu.VMEM((1024, XW), BF16), pltpu.VMEM((1024, XW), BF16)],
        n_in=5,
        flops=1 << 31,
        nbytes=1 << 23,
    )(sums, coding.T, alive.reshape(1, -1), xt, gt)
    parts = [parts[0]] + [shift(parts[k], "x", k) for k in (1, 2, 3)]
    tiles = call(add_up, [((16, GW), F32)] * 4, n_in=4, flops=1 << 16, nbytes=1 << 20)(*parts)
    tiles = [tiles[0]] + [shift(tiles[k], "zl", k) for k in (1, 2, 3)]
    (out,) = call(
        lay_out, [((16, columns), F32)], scratch=[pltpu.VMEM((16, 4 * GW), F32)], n_in=4, flops=1 << 16, nbytes=1 << 19
    )(*tiles)
    return out


def solution(mesh):
    finer = Mesh(mesh.devices.reshape(4, 4, 4, 2, 2), ALL)
    placed = (P(DP, "t"), P(DP, "t"), P(), P())
    return jax.shard_map(steps, mesh=finer, in_specs=placed, out_specs=P(DP, "t"), check_vma=False)
```

```python
import functools
import math

import jax
import jax.numpy as jnp
from jax import lax
from jax.experimental import pallas as pl
from jax.experimental.pallas import tpu as pltpu
from jax.sharding import Mesh
from jax.sharding import PartitionSpec as P

DP = ("x", "zl", "y", "c")
ALL = (*DP, "t")
BF16 = jnp.bfloat16
F32 = jnp.float32
ROWS = 128
SLOTS = 4
GROUP = 32
EDGE = SLOTS - 1
XW = 256
GW = 640
VMEM = pl.BlockSpec(memory_space=pltpu.VMEM)


def shift(value, axis, by):
    n = lax.axis_size(axis)
    return lax.ppermute(value, axis, [(i, (i + by) % n) for i in range(n)])


def swap(value, axis, by):
    return lax.ppermute(value, axis, [(i, i ^ by) for i in range(lax.axis_size(axis))])


def around(value, by):
    place = [(z % 4) * 2 + z // 4 for z in range(8)]
    return lax.ppermute(value, ("zl", "t"), [(place[z], place[(z + by) % 8]) for z in range(8)])


def dot(a, b, dims, **kw):
    return lax.dot_general(a, b, (dims, ((), ())), preferred_element_type=F32, **kw)


def call(kernel, outs, scratch=(), n_in=1, in_specs=None, flops=0, nbytes=0, mib=16):
    return pl.pallas_call(
        kernel,
        out_shape=[jax.ShapeDtypeStruct(s, d) for s, d in outs],
        in_specs=in_specs or [VMEM] * n_in,
        out_specs=[VMEM] * len(outs),
        scratch_shapes=list(scratch),
        cost_estimate=pl.CostEstimate(flops=flops, bytes_accessed=nbytes, transcendentals=0),
        compiler_params=pltpu.CompilerParams(vmem_limit_bytes=mib << 20),
    )


def split_x(x_ref, xc_ref):
    x = x_ref[...]
    width = x.shape[1]
    src = lax.broadcasted_iota(jnp.int32, (width, 128), 0)
    col = lax.broadcasted_iota(jnp.int32, (width, 128), 1)
    base = (col // 64) * 512 + ((col % 64) // 16) * 128 + col % 16
    for k in range(8):
        pick = jnp.where(src == base + 16 * k, 1.0, 0.0).astype(BF16)
        xc_ref[k] = dot(x, pick, ((1,), (0,))).astype(BF16)


def split_g(g_ref, *refs):
    gc, wide = refs[:4], refs[4]
    width = g_ref.shape[1]
    wide[:, :width] = g_ref[...]
    wide[:, width:] = jnp.zeros((ROWS, 4 * GW - width), BF16)
    zl = lax.axis_index("zl")
    for k in range(4):
        gc[k][...] = wide[:, pl.ds(pl.multiple_of((zl ^ k) * GW, 128), GW)]


def assemble(places, *refs):
    xs, gs = refs[: len(places[0])], refs[len(places[0]) : -4]
    xt, gt, out, keep = refs[-4:]
    zl, y, c = lax.axis_index("zl"), lax.axis_index("y"), lax.axis_index("c")
    z = lax.axis_index("t") * 4 + zl
    for (back, half), ref in zip(places[0], xs):
        at = (z - back + 8) % 8
        rows = pl.ds(pl.multiple_of((at % 4) * 1024 + half, 512), ref.shape[0])
        xt[rows, pl.ds(pl.multiple_of((at // 4) * 128, 128), 128)] = ref[...]
    for (back, first, other), ref in zip(places[1], gs):
        core = (c + other) % 2
        for k in range(ref.shape[0] // ROWS):
            at = (zl ^ (first + k)) * 8 + ((y - back + 4) % 4) * 2 + core
            gt[pl.ds(pl.multiple_of(at * ROWS, ROWS), ROWS), :] = ref[k * ROWS : (k + 1) * ROWS, :]
    for ref, at in ((out, c), (keep, 1 - c)):
        rows = pl.ds(pl.multiple_of(at * ((GROUP - EDGE) * ROWS), ROWS), EDGE * ROWS)
        ref[:, :XW] = xt[rows, :]
        ref[:, XW:] = gt[rows, :]


def block_sums(xa, xb, ga, gb):
    gram = dot(xa, xb, ((1,), (1,))) * dot(ga, gb, ((1,), (1,)))
    return jnp.sum(gram.reshape(-1, ROWS, gram.shape[1]), axis=1)


def inner_pairs(xt, gt, v_ref):
    v_ref[...] = jnp.zeros_like(v_ref)

    def step(rows, cols, first, count):
        sums = block_sums(xt[rows, :], xt[cols, :], gt[rows, :], gt[cols, :])
        for s in range(2):
            for r in range(count):
                d = count - 2 + s - r
                if 0 <= d < SLOTS:
                    v_ref[pl.ds(d * GROUP + first + r, 1), :] = sums[r : r + 1, s * ROWS : (s + 1) * ROWS]

    step(slice(0, 2 * ROWS), slice(0, 2 * ROWS), 0, 2)
    step(slice(0, 4 * ROWS), slice(2 * ROWS, 4 * ROWS), 0, 4)

    def body(j, carry):
        first = 2 * j - EDGE
        rows = pl.ds(pl.multiple_of(first * ROWS, ROWS), 5 * ROWS)
        step(rows, pl.ds(pl.multiple_of(2 * j * ROWS, ROWS), 2 * ROWS), first, 5)
        return carry

    lax.fori_loop(2, GROUP // 2, body, 0, unroll=2)


def edge_pairs(v_ref, keep, got, out_ref, v):
    v[...] = v_ref[...]
    first = lax.axis_index("c") == 0
    sums = block_sums(keep[:, :XW], got[:, :XW], keep[:, XW:], got[:, XW:])

    def pair(i, j):
        return sums[i : i + 1, j * ROWS : (j + 1) * ROWS]

    for e in range(EDGE):
        for f in range(e + 1):
            at = (EDGE + f - e) * GROUP + GROUP - EDGE + e
            v[at : at + 1, :] = jnp.where(first, pair(e, f), pair(f, e))
    total = dot(jnp.ones((8, ROWS), F32), v[...], ((1,), (1,)), precision=lax.Precision.HIGHEST)
    out_ref[...] = jnp.broadcast_to(total[0:1].reshape(1, 1, ROWS), out_ref.shape)


def weigh(size, r_ref, coding_ref, alive_ref, xt, gt, *refs):
    outs, (acc, hi, lo) = refs[:4], refs[4:]
    x = lax.axis_index("x")
    workers = ROWS
    limit = 8.0 * math.sqrt(ROWS)
    parts = r_ref[...].reshape(4, 16, 2, 2, 1, 128)
    even = jnp.sum(parts[:, :, 0], axis=(1, 2))
    odd = jnp.sum(parts[:, :, 1], axis=(1, 2))
    lane = lax.broadcasted_iota(jnp.int32, (8, 128), 1)
    edge = (lane % GROUP) + lane // GROUP >= GROUP

    def full(row):
        return jnp.broadcast_to(row, (8, 128))

    groups = [full(even[i]) + jnp.where(edge, full(odd[(i + 1) % 4]), full(odd[i])) for i in range(4)]

    def turn(value, by):
        by = by % 128
        return value if by == 0 else pltpu.roll(value, by, 1)

    pairs = []
    for d in range(SLOTS):
        value = jnp.zeros((8, 128), F32)
        for i in range(4):
            value = jnp.where(lane // GROUP == i, turn(groups[i], GROUP * (i - d)), value)
        pairs.append(value)
    coef = [full(coding_ref[s : s + 1, :].astype(F32)) for s in range(SLOTS)]
    squares = jnp.zeros((8, 128), F32)
    for s in range(SLOTS):
        for u in range(s, SLOTS):
            squares += (1.0 if u == s else 2.0) * coef[s] * coef[u] * turn(pairs[u - s], -s)
    squares = jnp.maximum(squares, 0.0)
    factor = jnp.minimum(1.0, limit / jnp.sqrt(squares / size + 1e-6))
    scaled = full(alive_ref[...].astype(F32)) * factor * (1.0 / (limit * math.sqrt(workers)))
    weights = jnp.zeros((8, 128), F32)
    for s in range(SLOTS):
        weights += turn(scaled * coef[s], s)
    mine = pltpu.roll(weights, ((4 - x) % 4) * GROUP, 1)
    acc[...] = jnp.zeros_like(acc)

    def chunk(i, mine):
        for q in range(8):
            rows = pl.ds(pl.multiple_of((i * 8 + q) * ROWS, ROWS), ROWS)
            value = xt[rows, :].astype(F32) * mine[0:1, q : q + 1]
            top = value.astype(BF16)
            hi[q * ROWS : (q + 1) * ROWS, :] = top
            lo[q * ROWS : (q + 1) * ROWS, :] = (value - top.astype(F32)).astype(BF16)
        g = gt[pl.ds(pl.multiple_of(i * 1024, 1024), 1024), :]
        acc[...] += dot(hi[...], g, ((0,), (0,))) + dot(lo[...], g, ((0,), (0,)))
        return pltpu.roll(mine, 120, 1)

    lax.fori_loop(0, 4, chunk, mine, unroll=2)
    for k in range(4):
        outs[k][...] = acc[pl.ds(pl.multiple_of(((x + k) % 4) * 64, 64), 64), :]


def add_up(a, b, c, d, *outs):
    zl = lax.axis_index("zl")
    for k in range(4):
        rows = pl.ds(pl.multiple_of((zl ^ k) * 16, 16), 16)
        outs[k][...] = a[rows, :] + b[rows, :] + c[rows, :] + d[rows, :]


def lay_out(*refs):
    parts, out_ref, wide = refs[:4], refs[4], refs[5]
    zl = lax.axis_index("zl")
    for k in range(4):
        wide[:, pl.ds(pl.multiple_of((zl ^ k) * GW, 128), GW)] = parts[k][...]
    out_ref[...] = wide[:, : out_ref.shape[1]]


def steps(activations, dgrad, coding, alive):
    size = float(activations.shape[1] * 2) * float(dgrad.shape[1] * 2)
    columns = dgrad.shape[1]
    gc = call(
        split_g, [((ROWS, GW), BF16)] * 4, scratch=[pltpu.VMEM((ROWS, 4 * GW), BF16)], flops=1 << 16, nbytes=1 << 21
    )(dgrad)
    (xc,) = call(split_x, [((8, ROWS, 128), BF16)], flops=1 << 28, nbytes=1 << 20)(activations)
    xa = functools.partial(lax.all_to_all, tiled=True)(xc, ("y", "c"), 0, 0).reshape(8 * ROWS, 128)
    g = [gc[0]] + [swap(gc[k], "zl", k) for k in (1, 2, 3)]
    near, late = jnp.concatenate(g[:2], axis=0), jnp.concatenate(g[2:], axis=0)
    pieces = {}
    for name, first, own in (("A", 0, near), ("B", 2, late)):
        pieces[f"own{name}"] = (own, 0, first)
        pieces[f"up{name}"] = (shift(own, "y", 1), 1, first)
        pieces[f"down{name}"] = (shift(own, "y", -1), 3, first)
    pieces["farA"] = (shift(pieces["upA"][0], "y", 1), 2, 0)
    pieces["farB"] = (shift(pieces["downB"][0], "y", -1), 2, 2)
    gs = [v for v, _, _ in pieces.values()]
    g_places = [(back, first, 0) for _, back, first in pieces.values()]
    gs += [shift(v, "c", 1) for (v, _, _) in pieces.values()]
    g_places += [(back, first, 1) for _, back, first in pieces.values()]
    xs, x_places = [xa], [(0, 0)]
    for sign, way in ((1, "up"), (-1, "down")):
        value = xa
        for step in range(1, 5):
            half = 0
            if step == 4:
                half = 0 if sign == 1 else 512
                value = value[half : half + 512]
            value = around(value, sign)
            xs.append(value)
            x_places.append(((sign * step) % 8, half))
    tokens, rim = GROUP * ROWS, EDGE * ROWS
    way = []
    for i in range(4):
        way += [(i * 2, (i + 3) % 4 * 2), (i * 2 + 1, (i + 1) % 4 * 2 + 1)]
    xt, gt, out, keep = call(
        functools.partial(assemble, (x_places, g_places)),
        [((tokens, XW), BF16), ((tokens, GW), BF16), ((rim, XW + GW), BF16), ((rim, XW + GW), BF16)],
        n_in=len(xs) + len(gs),
        nbytes=1 << 24,
    )(*xs, *gs)
    got = lax.ppermute(out, ("x", "c"), way)
    (v,) = call(inner_pairs, [((128, 128), F32)], n_in=2, flops=1 << 32, nbytes=1 << 23)(xt, gt)
    (sums,) = call(
        edge_pairs, [((256, 1, 128), F32)], scratch=[pltpu.VMEM((128, 128), F32)], n_in=3, flops=1 << 28, nbytes=1 << 20
    )(v, keep, got)
    sums = lax.all_to_all(sums, ALL, 0, 0, tiled=True)
    parts = call(
        functools.partial(weigh, size),
        [((64, GW), F32)] * 4,
        scratch=[pltpu.VMEM((XW, GW), F32), pltpu.VMEM((1024, XW), BF16), pltpu.VMEM((1024, XW), BF16)],
        n_in=5,
        flops=1 << 31,
        nbytes=1 << 23,
    )(sums, coding.T, alive.reshape(1, -1), xt, gt)
    parts = [parts[0]] + [shift(parts[k], "x", k) for k in (1, 2, 3)]
    tiles = call(add_up, [((16, GW), F32)] * 4, n_in=4, flops=1 << 16, nbytes=1 << 20)(*parts)
    tiles = [tiles[0]] + [swap(tiles[k], "zl", k) for k in (1, 2, 3)]
    (out,) = call(
        lay_out, [((16, columns), F32)], scratch=[pltpu.VMEM((16, 4 * GW), F32)], n_in=4, flops=1 << 16, nbytes=1 << 19
    )(*tiles)
    return out


def solution(mesh):
    finer = Mesh(mesh.devices.reshape(4, 4, 4, 2, 2), ALL)
    placed = (P(DP, "t"), P(DP, "t"), P(), P())
    return jax.shard_map(steps, mesh=finer, in_specs=placed, out_specs=P(DP, "t"), check_vma=False)
```

```python
import functools
import math

import jax
import jax.numpy as jnp
from jax import lax
from jax.experimental import pallas as pl
from jax.experimental.pallas import tpu as pltpu
from jax.sharding import Mesh
from jax.sharding import PartitionSpec as P

DP = ("x", "zl", "y", "c")
ALL = (*DP, "t")
BF16 = jnp.bfloat16
F32 = jnp.float32
ROWS = 128
SLOTS = 4
GROUP = 32
EDGE = SLOTS - 1
XW = 256
GW = 640
VMEM = pl.BlockSpec(memory_space=pltpu.VMEM)


def shift(value, axis, by):
    n = lax.axis_size(axis)
    return lax.ppermute(value, axis, [(i, (i + by) % n) for i in range(n)])


def swap(value, axis, by):
    return lax.ppermute(value, axis, [(i, i ^ by) for i in range(lax.axis_size(axis))])


def around(value, by):
    place = [(z % 4) * 2 + z // 4 for z in range(8)]
    return lax.ppermute(value, ("zl", "t"), [(place[z], place[(z + by) % 8]) for z in range(8)])


def dot(a, b, dims, **kw):
    return lax.dot_general(a, b, (dims, ((), ())), preferred_element_type=F32, **kw)


def call(kernel, outs, scratch=(), n_in=1, in_specs=None, flops=0, nbytes=0, mib=16):
    return pl.pallas_call(
        kernel,
        out_shape=[jax.ShapeDtypeStruct(s, d) for s, d in outs],
        in_specs=in_specs or [VMEM] * n_in,
        out_specs=[VMEM] * len(outs),
        scratch_shapes=list(scratch),
        cost_estimate=pl.CostEstimate(flops=flops, bytes_accessed=nbytes, transcendentals=0),
        compiler_params=pltpu.CompilerParams(vmem_limit_bytes=mib << 20),
    )


def split_x(x_ref, xc_ref):
    x = x_ref[...]
    width = x.shape[1]
    src = lax.broadcasted_iota(jnp.int32, (width, 128), 0)
    col = lax.broadcasted_iota(jnp.int32, (width, 128), 1)
    base = (col // 64) * 512 + ((col % 64) // 16) * 128 + col % 16
    for k in range(8):
        pick = jnp.where(src == base + 16 * k, 1.0, 0.0).astype(BF16)
        xc_ref[k] = dot(x, pick, ((1,), (0,))).astype(BF16)


def split_g(g_ref, *refs):
    gc, wide = refs[:4], refs[4]
    width = g_ref.shape[1]
    wide[:, :width] = g_ref[...]
    wide[:, width:] = jnp.zeros((ROWS, 4 * GW - width), BF16)
    zl = lax.axis_index("zl")
    for k in range(4):
        gc[k][...] = wide[:, pl.ds(pl.multiple_of((zl ^ k) * GW, 128), GW)]


def edges(tile, out_ref, keep_ref):
    c = lax.axis_index("c")
    for ref, at in ((out_ref, c), (keep_ref, 1 - c)):
        ref[...] = tile[pl.ds(pl.multiple_of(at * ((GROUP - EDGE) * ROWS), ROWS), EDGE * ROWS), :]


def assemble_x(places, *refs):
    xt = refs[-3]
    z = lax.axis_index("t") * 4 + lax.axis_index("zl")
    for (back, half), ref in zip(places, refs[:-3]):
        at = (z - back + 8) % 8
        rows = pl.ds(pl.multiple_of((at % 4) * 1024 + half, 512), ref.shape[0])
        xt[rows, pl.ds(pl.multiple_of((at // 4) * 128, 128), 128)] = ref[...]
    edges(*refs[-3:])


def assemble_g(places, *refs):
    gt = refs[-3]
    zl, y, c = lax.axis_index("zl"), lax.axis_index("y"), lax.axis_index("c")
    for (back, first, other), ref in zip(places, refs[:-3]):
        core = (c + other) % 2
        for k in range(ref.shape[0] // ROWS):
            at = (zl ^ (first + k)) * 8 + ((y - back + 4) % 4) * 2 + core
            gt[pl.ds(pl.multiple_of(at * ROWS, ROWS), ROWS), :] = ref[k * ROWS : (k + 1) * ROWS, :]
    edges(*refs[-3:])


def block_sums(gram):
    return jnp.sum(gram.reshape(-1, ROWS, gram.shape[1]), axis=1)


def over_pairs(step):
    step(0, slice(0, 2 * ROWS), slice(0, 2 * ROWS), 0, 2)
    step(1, slice(0, 4 * ROWS), slice(2 * ROWS, 4 * ROWS), 0, 4)

    def body(j, carry):
        first = 2 * j - EDGE
        rows = pl.ds(pl.multiple_of(first * ROWS, ROWS), 5 * ROWS)
        step(j, rows, pl.ds(pl.multiple_of(2 * j * ROWS, ROWS), 2 * ROWS), first, 5)
        return carry

    lax.fori_loop(2, GROUP // 2, body, 0, unroll=2)


def g_grams(gt, out_ref):
    def step(j, rows, cols, first, count):
        out_ref[j, : count * ROWS, :] = dot(gt[rows, :], gt[cols, :], ((1,), (1,)))

    over_pairs(step)


def inner_pairs(xt, grams, v_ref):
    v_ref[...] = jnp.zeros_like(v_ref)

    def step(j, rows, cols, first, count):
        sums = block_sums(dot(xt[rows, :], xt[cols, :], ((1,), (1,))) * grams[j, : count * ROWS, :])
        for s in range(2):
            for r in range(count):
                d = count - 2 + s - r
                if 0 <= d < SLOTS:
                    v_ref[pl.ds(d * GROUP + first + r, 1), :] = sums[r : r + 1, s * ROWS : (s + 1) * ROWS]

    over_pairs(step)


def edge_pairs(v_ref, keep_x, got_x, keep_g, got_g, out_ref, v):
    v[...] = v_ref[...]
    first = lax.axis_index("c") == 0
    grams = [dot(a[...], b[...], ((1,), (1,))) for a, b in ((keep_x, got_x), (keep_g, got_g))]
    sums = block_sums(grams[0] * grams[1])

    def pair(i, j):
        return sums[i : i + 1, j * ROWS : (j + 1) * ROWS]

    for e in range(EDGE):
        for f in range(e + 1):
            at = (EDGE + f - e) * GROUP + GROUP - EDGE + e
            v[at : at + 1, :] = jnp.where(first, pair(e, f), pair(f, e))
    total = dot(jnp.ones((8, ROWS), F32), v[...], ((1,), (1,)), precision=lax.Precision.HIGHEST)
    out_ref[...] = jnp.broadcast_to(total[0:1].reshape(1, 1, ROWS), out_ref.shape)


def weigh(size, r_ref, coding_ref, alive_ref, xt, gt, *refs):
    outs, (acc, hi, lo) = refs[:4], refs[4:]
    x = lax.axis_index("x")
    workers = ROWS
    limit = 8.0 * math.sqrt(ROWS)
    parts = r_ref[...].reshape(4, 16, 2, 2, 1, 128)
    even = jnp.sum(parts[:, :, 0], axis=(1, 2))
    odd = jnp.sum(parts[:, :, 1], axis=(1, 2))
    lane = lax.broadcasted_iota(jnp.int32, (8, 128), 1)
    edge = (lane % GROUP) + lane // GROUP >= GROUP

    def full(row):
        return jnp.broadcast_to(row, (8, 128))

    groups = [full(even[i]) + jnp.where(edge, full(odd[(i + 1) % 4]), full(odd[i])) for i in range(4)]

    def turn(value, by):
        by = by % 128
        return value if by == 0 else pltpu.roll(value, by, 1)

    pairs = []
    for d in range(SLOTS):
        value = jnp.zeros((8, 128), F32)
        for i in range(4):
            value = jnp.where(lane // GROUP == i, turn(groups[i], GROUP * (i - d)), value)
        pairs.append(value)
    coef = [full(coding_ref[s : s + 1, :].astype(F32)) for s in range(SLOTS)]
    squares = jnp.zeros((8, 128), F32)
    for s in range(SLOTS):
        for u in range(s, SLOTS):
            squares += (1.0 if u == s else 2.0) * coef[s] * coef[u] * turn(pairs[u - s], -s)
    squares = jnp.maximum(squares, 0.0)
    factor = jnp.minimum(1.0, limit / jnp.sqrt(squares / size + 1e-6))
    scaled = full(alive_ref[...].astype(F32)) * factor * (1.0 / (limit * math.sqrt(workers)))
    weights = jnp.zeros((8, 128), F32)
    for s in range(SLOTS):
        weights += turn(scaled * coef[s], s)
    mine = pltpu.roll(weights, ((4 - x) % 4) * GROUP, 1)
    acc[...] = jnp.zeros_like(acc)

    def chunk(i, mine):
        for q in range(8):
            rows = pl.ds(pl.multiple_of((i * 8 + q) * ROWS, ROWS), ROWS)
            value = xt[rows, :].astype(F32) * mine[0:1, q : q + 1]
            top = value.astype(BF16)
            hi[q * ROWS : (q + 1) * ROWS, :] = top
            lo[q * ROWS : (q + 1) * ROWS, :] = (value - top.astype(F32)).astype(BF16)
        g = gt[pl.ds(pl.multiple_of(i * 1024, 1024), 1024), :]
        acc[...] += dot(hi[...], g, ((0,), (0,))) + dot(lo[...], g, ((0,), (0,)))
        return pltpu.roll(mine, 120, 1)

    lax.fori_loop(0, 4, chunk, mine, unroll=4)
    for k in range(4):
        outs[k][...] = acc[pl.ds(pl.multiple_of(((x + k) % 4) * 64, 64), 64), :]


def add_up(a, b, c, d, *outs):
    zl = lax.axis_index("zl")
    for k in range(4):
        rows = pl.ds(pl.multiple_of((zl ^ k) * 16, 16), 16)
        outs[k][...] = a[rows, :] + b[rows, :] + c[rows, :] + d[rows, :]


def lay_out(*refs):
    parts, out_ref, wide = refs[:4], refs[4], refs[5]
    zl = lax.axis_index("zl")
    for k in range(4):
        wide[:, pl.ds(pl.multiple_of((zl ^ k) * GW, 128), GW)] = parts[k][...]
    out_ref[...] = wide[:, : out_ref.shape[1]]


def steps(activations, dgrad, coding, alive):
    size = float(activations.shape[1] * 2) * float(dgrad.shape[1] * 2)
    columns = dgrad.shape[1]
    gc = call(
        split_g, [((ROWS, GW), BF16)] * 4, scratch=[pltpu.VMEM((ROWS, 4 * GW), BF16)], flops=1 << 16, nbytes=1 << 21
    )(dgrad)
    (xc,) = call(split_x, [((8, ROWS, 128), BF16)], flops=1 << 28, nbytes=1 << 20)(activations)
    xa = functools.partial(lax.all_to_all, tiled=True)(xc, ("y", "c"), 0, 0).reshape(8 * ROWS, 128)
    g = [gc[0]] + [swap(gc[k], "zl", k) for k in (1, 2, 3)]
    near, late = jnp.concatenate(g[:2], axis=0), jnp.concatenate(g[2:], axis=0)
    pieces = {}
    for name, first, own in (("A", 0, near), ("B", 2, late)):
        pieces[f"own{name}"] = (own, 0, first)
        pieces[f"up{name}"] = (shift(own, "y", 1), 1, first)
        pieces[f"down{name}"] = (shift(own, "y", -1), 3, first)
    pieces["farA"] = (shift(pieces["upA"][0], "y", 1), 2, 0)
    pieces["farB"] = (shift(pieces["downB"][0], "y", -1), 2, 2)
    gs = [v for v, _, _ in pieces.values()]
    g_places = [(back, first, 0) for _, back, first in pieces.values()]
    gs += [shift(v, "c", 1) for (v, _, _) in pieces.values()]
    g_places += [(back, first, 1) for _, back, first in pieces.values()]
    xs, x_places = [xa], [(0, 0)]
    for sign, way in ((1, "up"), (-1, "down")):
        value = xa
        for step in range(1, 5):
            half = 0
            if step == 4:
                half = 0 if sign == 1 else 512
                value = value[half : half + 512]
            value = around(value, sign)
            xs.append(value)
            x_places.append(((sign * step) % 8, half))
    tokens, rim = GROUP * ROWS, EDGE * ROWS
    way = []
    for i in range(4):
        way += [(i * 2, (i + 3) % 4 * 2), (i * 2 + 1, (i + 1) % 4 * 2 + 1)]
    gt, out_g, keep_g = call(
        functools.partial(assemble_g, g_places),
        [((tokens, GW), BF16), ((rim, GW), BF16), ((rim, GW), BF16)],
        n_in=len(gs),
        nbytes=1 << 24,
    )(*gs)
    got_g = lax.ppermute(out_g, ("x", "c"), way)
    (grams,) = call(g_grams, [((GROUP // 2, 5 * ROWS, 2 * ROWS), F32)], flops=1 << 32, nbytes=1 << 24)(gt)
    xt, out_x, keep_x = call(
        functools.partial(assemble_x, x_places),
        [((tokens, XW), BF16), ((rim, XW), BF16), ((rim, XW), BF16)],
        n_in=len(xs),
        nbytes=1 << 22,
    )(*xs)
    got_x = lax.ppermute(out_x, ("x", "c"), way)
    (v,) = call(inner_pairs, [((128, 128), F32)], n_in=2, flops=1 << 31, nbytes=1 << 24)(xt, grams)
    (sums,) = call(
        edge_pairs, [((256, 1, 128), F32)], scratch=[pltpu.VMEM((128, 128), F32)], n_in=5, flops=1 << 28, nbytes=1 << 20
    )(v, keep_x, got_x, keep_g, got_g)
    sums = lax.all_to_all(sums, ALL, 0, 0, tiled=True)
    parts = call(
        functools.partial(weigh, size),
        [((64, GW), F32)] * 4,
        scratch=[pltpu.VMEM((XW, GW), F32), pltpu.VMEM((1024, XW), BF16), pltpu.VMEM((1024, XW), BF16)],
        n_in=5,
        flops=1 << 31,
        nbytes=1 << 23,
    )(sums, coding.T, alive.reshape(1, -1), xt, gt)
    parts = [parts[0]] + [shift(parts[k], "x", k) for k in (1, 2, 3)]
    tiles = call(add_up, [((16, GW), F32)] * 4, n_in=4, flops=1 << 16, nbytes=1 << 20)(*parts)
    tiles = [tiles[0]] + [swap(tiles[k], "zl", k) for k in (1, 2, 3)]
    (out,) = call(
        lay_out, [((16, columns), F32)], scratch=[pltpu.VMEM((16, 4 * GW), F32)], n_in=4, flops=1 << 16, nbytes=1 << 19
    )(*tiles)
    return out


def solution(mesh):
    finer = Mesh(mesh.devices.reshape(4, 4, 4, 2, 2), ALL)
    placed = (P(DP, "t"), P(DP, "t"), P(), P())
    return jax.shard_map(steps, mesh=finer, in_specs=placed, out_specs=P(DP, "t"), check_vma=False)
```

```python
import functools
import math

import jax
import jax.numpy as jnp
from jax import lax
from jax.experimental import pallas as pl
from jax.experimental.pallas import tpu as pltpu
from jax.sharding import Mesh
from jax.sharding import PartitionSpec as P

DP = ("x", "zl", "y", "c")
ALL = (*DP, "t")
BF16 = jnp.bfloat16
F32 = jnp.float32
ROWS = 128
SLOTS = 4
GROUP = 32
EDGE = SLOTS - 1
XW = 256
GW = 640
VMEM = pl.BlockSpec(memory_space=pltpu.VMEM)


def shift(value, axis, by):
    n = lax.axis_size(axis)
    return lax.ppermute(value, axis, [(i, (i + by) % n) for i in range(n)])


def swap(value, axis, by):
    return lax.ppermute(value, axis, [(i, i ^ by) for i in range(lax.axis_size(axis))])


def around(value, by):
    place = [(z % 4) * 2 + z // 4 for z in range(8)]
    return lax.ppermute(value, ("zl", "t"), [(place[z], place[(z + by) % 8]) for z in range(8)])


def dot(a, b, dims, **kw):
    return lax.dot_general(a, b, (dims, ((), ())), preferred_element_type=F32, **kw)


def call(kernel, outs, scratch=(), n_in=1, in_specs=None, flops=0, nbytes=0, mib=16):
    return pl.pallas_call(
        kernel,
        out_shape=[jax.ShapeDtypeStruct(s, d) for s, d in outs],
        in_specs=in_specs or [VMEM] * n_in,
        out_specs=[VMEM] * len(outs),
        scratch_shapes=list(scratch),
        cost_estimate=pl.CostEstimate(flops=flops, bytes_accessed=nbytes, transcendentals=0),
        compiler_params=pltpu.CompilerParams(vmem_limit_bytes=mib << 20),
    )


def split_x(x_ref, xc_ref):
    x = x_ref[...]
    width = x.shape[1]
    src = lax.broadcasted_iota(jnp.int32, (width, 128), 0)
    col = lax.broadcasted_iota(jnp.int32, (width, 128), 1)
    base = (col // 64) * 512 + ((col % 64) // 16) * 128 + col % 16
    for k in range(8):
        pick = jnp.where(src == base + 16 * k, 1.0, 0.0).astype(BF16)
        xc_ref[k] = dot(x, pick, ((1,), (0,))).astype(BF16)


def split_g(g_ref, *refs):
    gc, wide = refs[:4], refs[4]
    width = g_ref.shape[1]
    wide[:, :width] = g_ref[...]
    wide[:, width:] = jnp.zeros((ROWS, 4 * GW - width), BF16)
    zl = lax.axis_index("zl")
    for k in range(4):
        gc[k][...] = wide[:, pl.ds(pl.multiple_of((zl ^ k) * GW, 128), GW)]


def edges(tile, out_ref, keep_ref):
    c = lax.axis_index("c")
    for ref, at in ((out_ref, c), (keep_ref, 1 - c)):
        ref[...] = tile[pl.ds(pl.multiple_of(at * ((GROUP - EDGE) * ROWS), ROWS), EDGE * ROWS), :]


def assemble_x(places, *refs):
    xt = refs[-3]
    z = lax.axis_index("t") * 4 + lax.axis_index("zl")
    for (back, half), ref in zip(places, refs[:-3]):
        at = (z - back + 8) % 8
        rows = pl.ds(pl.multiple_of((at % 4) * 1024 + half, 512), ref.shape[0])
        xt[rows, pl.ds(pl.multiple_of((at // 4) * 128, 128), 128)] = ref[...]
    edges(*refs[-3:])


def assemble_g(places, *refs):
    gt = refs[-3]
    zl, y, c = lax.axis_index("zl"), lax.axis_index("y"), lax.axis_index("c")
    for (back, first, other), ref in zip(places, refs[:-3]):
        core = (c + other) % 2
        for k in range(ref.shape[0] // ROWS):
            at = (zl ^ (first + k)) * 8 + ((y - back + 4) % 4) * 2 + core
            gt[pl.ds(pl.multiple_of(at * ROWS, ROWS), ROWS), :] = ref[k * ROWS : (k + 1) * ROWS, :]
    edges(*refs[-3:])


def block_sums(gram):
    return jnp.sum(gram.reshape(-1, ROWS, gram.shape[1]), axis=1)


def over_pairs(step):
    step(0, slice(0, 2 * ROWS), slice(0, 2 * ROWS), 0, 2)
    step(1, slice(0, 4 * ROWS), slice(2 * ROWS, 4 * ROWS), 0, 4)

    def body(j, carry):
        first = 2 * j - EDGE
        rows = pl.ds(pl.multiple_of(first * ROWS, ROWS), 5 * ROWS)
        step(j, rows, pl.ds(pl.multiple_of(2 * j * ROWS, ROWS), 2 * ROWS), first, 5)
        return carry

    lax.fori_loop(2, GROUP // 2, body, 0, unroll=2)


def g_grams(gt, out_ref):
    def step(j, rows, cols, first, count):
        out_ref[j, : count * ROWS, :] = dot(gt[rows, :], gt[cols, :], ((1,), (1,)))

    over_pairs(step)


def inner_pairs(xt, grams, v_ref):
    v_ref[...] = jnp.zeros_like(v_ref)

    def step(j, rows, cols, first, count):
        sums = block_sums(dot(xt[rows, :], xt[cols, :], ((1,), (1,))) * grams[j, : count * ROWS, :])
        for s in range(2):
            for r in range(count):
                d = count - 2 + s - r
                if 0 <= d < SLOTS:
                    v_ref[pl.ds(d * GROUP + first + r, 1), :] = sums[r : r + 1, s * ROWS : (s + 1) * ROWS]

    over_pairs(step)


def edge_pairs(v_ref, keep_x, got_x, keep_g, got_g, out_ref, v):
    v[...] = v_ref[...]
    first = lax.axis_index("c") == 0
    grams = [dot(a[...], b[...], ((1,), (1,))) for a, b in ((keep_x, got_x), (keep_g, got_g))]
    sums = block_sums(grams[0] * grams[1])

    def pair(i, j):
        return sums[i : i + 1, j * ROWS : (j + 1) * ROWS]

    for e in range(EDGE):
        for f in range(e + 1):
            at = (EDGE + f - e) * GROUP + GROUP - EDGE + e
            v[at : at + 1, :] = jnp.where(first, pair(e, f), pair(f, e))
    total = dot(jnp.ones((8, ROWS), F32), v[...], ((1,), (1,)), precision=lax.Precision.HIGHEST)
    out_ref[...] = jnp.broadcast_to(total[0:1].reshape(1, 1, ROWS), out_ref.shape)


def weigh(size, r_ref, coding_ref, alive_ref, xt, gt, *refs):
    outs, (acc, hi, lo) = refs[:4], refs[4:]
    x = lax.axis_index("x")
    workers = ROWS
    limit = 8.0 * math.sqrt(ROWS)
    parts = r_ref[...].reshape(4, 16, 2, 2, 1, 128)
    even = jnp.sum(parts[:, :, 0], axis=(1, 2))
    odd = jnp.sum(parts[:, :, 1], axis=(1, 2))
    lane = lax.broadcasted_iota(jnp.int32, (8, 128), 1)
    edge = (lane % GROUP) + lane // GROUP >= GROUP

    def full(row):
        return jnp.broadcast_to(row, (8, 128))

    groups = [full(even[i]) + jnp.where(edge, full(odd[(i + 1) % 4]), full(odd[i])) for i in range(4)]

    def turn(value, by):
        by = by % 128
        return value if by == 0 else pltpu.roll(value, by, 1)

    pairs = []
    for d in range(SLOTS):
        value = jnp.zeros((8, 128), F32)
        for i in range(4):
            value = jnp.where(lane // GROUP == i, turn(groups[i], GROUP * (i - d)), value)
        pairs.append(value)
    coef = [full(coding_ref[s : s + 1, :].astype(F32)) for s in range(SLOTS)]
    squares = jnp.zeros((8, 128), F32)
    for s in range(SLOTS):
        for u in range(s, SLOTS):
            squares += (1.0 if u == s else 2.0) * coef[s] * coef[u] * turn(pairs[u - s], -s)
    squares = jnp.maximum(squares, 0.0)
    factor = jnp.minimum(1.0, limit / jnp.sqrt(squares / size + 1e-6))
    scaled = full(alive_ref[...].astype(F32)) * factor * (1.0 / (limit * math.sqrt(workers)))
    weights = jnp.zeros((8, 128), F32)
    for s in range(SLOTS):
        weights += turn(scaled * coef[s], s)
    mine = pltpu.roll(weights, ((4 - x) % 4) * GROUP, 1)
    acc[...] = jnp.zeros_like(acc)

    def chunk(i, mine):
        for q in range(8):
            rows = pl.ds(pl.multiple_of((i * 8 + q) * ROWS, ROWS), ROWS)
            value = xt[rows, :].astype(F32) * mine[0:1, q : q + 1]
            top = value.astype(BF16)
            hi[q * ROWS : (q + 1) * ROWS, :] = top
            lo[q * ROWS : (q + 1) * ROWS, :] = (value - top.astype(F32)).astype(BF16)
        g = gt[pl.ds(pl.multiple_of(i * 1024, 1024), 1024), :]
        acc[...] += dot(hi[...], g, ((0,), (0,))) + dot(lo[...], g, ((0,), (0,)))
        return pltpu.roll(mine, 120, 1)

    lax.fori_loop(0, 4, chunk, mine, unroll=4)
    for k in range(4):
        outs[k][...] = acc[pl.ds(pl.multiple_of(((x + k) % 4) * 64, 64), 64), :]


def add_up(a, b, c, d, *outs):
    zl = lax.axis_index("zl")
    for k in range(4):
        rows = pl.ds(pl.multiple_of((zl ^ k) * 16, 16), 16)
        outs[k][...] = a[rows, :] + b[rows, :] + c[rows, :] + d[rows, :]


def lay_out(*refs):
    parts, out_ref, wide = refs[:4], refs[4], refs[5]
    zl = lax.axis_index("zl")
    for k in range(4):
        wide[:, pl.ds(pl.multiple_of((zl ^ k) * GW, 128), GW)] = parts[k][...]
    out_ref[...] = wide[:, : out_ref.shape[1]]


def steps(activations, dgrad, coding, alive):
    size = float(activations.shape[1] * 2) * float(dgrad.shape[1] * 2)
    columns = dgrad.shape[1]
    gc = call(
        split_g, [((ROWS, GW), BF16)] * 4, scratch=[pltpu.VMEM((ROWS, 4 * GW), BF16)], flops=1 << 16, nbytes=1 << 21
    )(dgrad)
    (xc,) = call(split_x, [((8, ROWS, 128), BF16)], flops=1 << 28, nbytes=1 << 20)(activations)
    xa = functools.partial(lax.all_to_all, tiled=True)(xc, ("y", "c"), 0, 0).reshape(8 * ROWS, 128)
    g = [gc[0]] + [swap(gc[k], "zl", k) for k in (1, 2, 3)]
    own = jnp.concatenate(g, axis=0)
    up, down = shift(own, "y", 1), shift(own, "y", -1)
    pieces = {
        "own": (own, 0, 0),
        "up": (up, 1, 0),
        "down": (down, 3, 0),
        "farA": (shift(up[: 2 * ROWS], "y", 1), 2, 0),
        "farB": (shift(down[2 * ROWS :], "y", -1), 2, 2),
    }
    gs = [v for v, _, _ in pieces.values()]
    g_places = [(back, first, 0) for _, back, first in pieces.values()]
    gs += [shift(v, "c", 1) for (v, _, _) in pieces.values()]
    g_places += [(back, first, 1) for _, back, first in pieces.values()]
    xs, x_places = [xa], [(0, 0)]
    for sign, way in ((1, "up"), (-1, "down")):
        value = xa
        for step in range(1, 5):
            half = 0
            if step == 4:
                half = 0 if sign == 1 else 512
                value = value[half : half + 512]
            value = around(value, sign)
            xs.append(value)
            x_places.append(((sign * step) % 8, half))
    tokens, rim = GROUP * ROWS, EDGE * ROWS
    way = []
    for i in range(4):
        way += [(i * 2, (i + 3) % 4 * 2), (i * 2 + 1, (i + 1) % 4 * 2 + 1)]
    gt, out_g, keep_g = call(
        functools.partial(assemble_g, g_places),
        [((tokens, GW), BF16), ((rim, GW), BF16), ((rim, GW), BF16)],
        n_in=len(gs),
        nbytes=1 << 24,
    )(*gs)
    got_g = lax.ppermute(out_g, ("x", "c"), way)
    (grams,) = call(g_grams, [((GROUP // 2, 5 * ROWS, 2 * ROWS), F32)], flops=1 << 32, nbytes=1 << 24)(gt)
    xt, out_x, keep_x = call(
        functools.partial(assemble_x, x_places),
        [((tokens, XW), BF16), ((rim, XW), BF16), ((rim, XW), BF16)],
        n_in=len(xs),
        nbytes=1 << 22,
    )(*xs)
    got_x = lax.ppermute(out_x, ("x", "c"), way)
    (v,) = call(inner_pairs, [((128, 128), F32)], n_in=2, flops=1 << 31, nbytes=1 << 24)(xt, grams)
    (sums,) = call(
        edge_pairs, [((256, 1, 128), F32)], scratch=[pltpu.VMEM((128, 128), F32)], n_in=5, flops=1 << 28, nbytes=1 << 20
    )(v, keep_x, got_x, keep_g, got_g)
    sums = lax.all_to_all(sums, ALL, 0, 0, tiled=True)
    parts = call(
        functools.partial(weigh, size),
        [((64, GW), F32)] * 4,
        scratch=[pltpu.VMEM((XW, GW), F32), pltpu.VMEM((1024, XW), BF16), pltpu.VMEM((1024, XW), BF16)],
        n_in=5,
        flops=1 << 31,
        nbytes=1 << 23,
    )(sums, coding.T, alive.reshape(1, -1), xt, gt)
    parts = [parts[0]] + [shift(parts[k], "x", k) for k in (1, 2, 3)]
    tiles = call(add_up, [((16, GW), F32)] * 4, n_in=4, flops=1 << 16, nbytes=1 << 20)(*parts)
    tiles = [tiles[0]] + [swap(tiles[k], "zl", k) for k in (1, 2, 3)]
    (out,) = call(
        lay_out, [((16, columns), F32)], scratch=[pltpu.VMEM((16, 4 * GW), F32)], n_in=4, flops=1 << 16, nbytes=1 << 19
    )(*tiles)
    return out


def solution(mesh):
    finer = Mesh(mesh.devices.reshape(4, 4, 4, 2, 2), ALL)
    placed = (P(DP, "t"), P(DP, "t"), P(), P())
    return jax.shard_map(steps, mesh=finer, in_specs=placed, out_specs=P(DP, "t"), check_vma=False)
```
